32 devices in a mesh: seq: 8 (over y, x, core), chan: 4 (over z).
Axes of the slice: x: 2, y: 2, z: 4, core: 2. Of those that a mesh axis runs over, the one named last changes fastest.
Arguments:
- fwd_q: bfloat16 [1024, 4096], P('seq', 'chan'), may hold values from -6 to 6
- fwd_k: bfloat16 [1024, 4096], P('seq', 'chan'), may hold values from -6 to 6
- fwd_v: bfloat16 [1024, 4096], P('seq', 'chan'), may hold values from -6 to 6
- bwd_q: bfloat16 [1024, 4096], P('seq', 'chan'), may hold values from -6 to 6
- bwd_k: bfloat16 [1024, 4096], P('seq', 'chan'), may hold values from -6 to 6
- bwd_v: bfloat16 [1024, 4096], P('seq', 'chan'), may hold values from -6 to 6
- bwd_grad: bfloat16 [1024, 4096], P('seq', 'chan'), may hold values from -6 to 6
- filters: float32 [1024, 1024], P('seq', 'chan'), may hold values from -0.1875 to 0.1875
- skip: float32 [4096], P('chan'), may hold values from -4 to 4
Outputs:
- output: bfloat16 [1024, 4096], P('seq', 'chan')
- grad_query: bfloat16 [1024, 4096], P('seq', 'chan')
- grad_key: bfloat16 [1024, 4096], P('seq', 'chan')
- grad_value: bfloat16 [1024, 4096], P('seq', 'chan')
- grad_filter: float32 [1024, 1024], P('seq', 'chan')
- grad_skip: float32 [4096], P('chan')
The draws below stay inside these ranges and needn't reach their ends.
All inputs are finite; a program needn't handle non-finite values.
Results may differ from the reference program's by a relative error of at most 0.0075.
Values may be sent and summed in bfloat16 or wider, within the bound.
No kernel may reach another device: no remote copies, remote signals or barrier semaphores. Data moves between devices by JAX's collectives and lax.ppermute only.
A program may use at most 256 MiB of HBM per device.

```python
import math
import jax
import jax.numpy as jnp
from jax import lax

C = 4096
FILTERS = 1024
SEQ_LEN = 1024


def block_scale(key, shape, shards, smallest, top_value):
    gain, own = 1.0, jax.random.fold_in(key, 6)
    for position, shards_of in shards:
        draws = jnp.exp(jax.random.uniform(jax.random.fold_in(own, position), (shards_of,), jnp.float32, smallest / len(shards), top_value / len(shards)))
        gain = gain * jnp.repeat(draws, shape[position] // shards_of).reshape([-1 if axis == position else 1 for axis in range(len(shape))])
    return gain


def bell_draw(own_key, extent, scale, limit, shards=(), kind=jnp.bfloat16):
    drawn = jax.random.normal(own_key, extent, jnp.float32) * scale
    if len(shards) > 0:
        drawn = block_scale(own_key, extent, shards, -0.22, 0.18) * drawn
    return jnp.clip(drawn, min=-limit, max=limit).astype(kind)


def setup_inputs(seed: int = 0) -> dict:
    streams_of = jax.random.split(jax.random.key(seed), 10)
    fwd_q = bell_draw(streams_of[0], (SEQ_LEN, C), 1.0, 6.0, ((0, 8), (1, 4)))
    fwd_k = bell_draw(streams_of[1], (SEQ_LEN, C), 1.0, 6.0, ((0, 8), (1, 4)))
    fwd_v = bell_draw(streams_of[2], (SEQ_LEN, C), 1.0, 6.0, ((0, 8), (1, 4)))
    bwd_q = bell_draw(streams_of[3], (SEQ_LEN, C), 1.0, 6.0, ((0, 8), (1, 4)))
    bwd_k = bell_draw(streams_of[4], (SEQ_LEN, C), 1.0, 6.0, ((0, 8), (1, 4)))
    bwd_v = bell_draw(streams_of[5], (SEQ_LEN, C), 1.0, 6.0, ((0, 8), (1, 4)))
    bwd_grad = bell_draw(streams_of[6], (SEQ_LEN, C), 1.0, 6.0, ((0, 8), (1, 4)))
    filters = bell_draw(streams_of[7], (SEQ_LEN, FILTERS), SEQ_LEN ** -0.5, 0.1875, ((0, 8), (1, 4)), jnp.float32)
    skip = bell_draw(streams_of[8], (C,), 1.0, 4.0, ((0, 4),), jnp.float32)
    return {"fwd_q": fwd_q, "fwd_k": fwd_k, "fwd_v": fwd_v, "bwd_q": bwd_q, "bwd_k": bwd_k, "bwd_v": bwd_v, "bwd_grad": bwd_grad, "filters": filters, "skip": skip}


def spectrum(values):
    return jnp.fft.rfft(values, n=2 * values.shape[0], axis=0)

def signal(spec, seq_length):
    return jnp.fft.irfft(spec, n=2 * seq_length, axis=0)[:seq_length]

def rounded(values):
    return lax.optimization_barrier(values.astype(jnp.bfloat16)).astype(jnp.float32)

def reference(fwd_q, fwd_k, fwd_v, bwd_q, bwd_k, bwd_v, bwd_grad, filters, skip):
    seq_length, channels = fwd_q.shape
    filter_count = filters.shape[1]
    grad_scale = 1.0 / math.sqrt(seq_length)
    filter_spec = spectrum(filters.astype(jnp.float32))
    out_parts, query_parts, key_parts, value_parts, skip_parts = ([], [], [], [], [])
    filter_total = jnp.zeros((seq_length, filter_count), jnp.float32)
    for group_index in range(channels // filter_count):
        start_col = group_index * filter_count
        stop_col = start_col + filter_count

        def column_block(array):
            return array[:, start_col:stop_col].astype(jnp.float32)
        skip_gain = skip[start_col:stop_col].astype(jnp.float32)
        source = rounded(column_block(fwd_k) * column_block(fwd_v))
        mixed = signal(filter_spec * spectrum(source), seq_length) + skip_gain * source
        out_parts.append((column_block(fwd_q) * mixed).astype(jnp.bfloat16))
        second_source = rounded(column_block(bwd_k) * column_block(bwd_v))
        second_spec = spectrum(second_source)
        mixed_two = signal(filter_spec * second_spec, seq_length) + skip_gain * second_source
        query_parts.append((column_block(bwd_grad) * mixed_two).astype(jnp.bfloat16))
        upstream = rounded(column_block(bwd_grad) * column_block(bwd_q))
        upstream_spec = spectrum(upstream)
        through = signal(jnp.conj(filter_spec) * upstream_spec, seq_length) + skip_gain * upstream
        key_parts.append((through * column_block(bwd_v)).astype(jnp.bfloat16))
        value_parts.append((through * column_block(bwd_k)).astype(jnp.bfloat16))
        filter_total = filter_total + signal(jnp.conj(second_spec) * upstream_spec, seq_length) * grad_scale
        skip_parts.append(lax.optimization_barrier(jnp.sum(upstream * second_source, axis=0)) * grad_scale)
    return (jnp.concatenate(out_parts, axis=1), jnp.concatenate(query_parts, axis=1), jnp.concatenate(key_parts, axis=1), jnp.concatenate(value_parts, axis=1), filter_total, jnp.concatenate(skip_parts, axis=0))
```

```python
import math

import jax
import jax.numpy as jnp
from jax import lax
from jax.experimental import pallas as pl
from jax.experimental.pallas import tpu as pltpu
from jax.sharding import PartitionSpec as P


HIGHEST = lax.Precision.HIGHEST


def index_ramp(total):
    return jnp.arange(total, dtype=jnp.int32)


def widened(values):
    return values.astype(jnp.float32)


def angles(out_index, in_index, period, sign):
    phase_steps = out_index[:, None] * in_index[None, :] % period
    phase = phase_steps.astype(jnp.float32) * (sign * 2.0 * math.pi / period)
    return (jnp.cos(phase), jnp.sin(phase))


def times_table(left, right):
    return (left[0] * right[0] - left[1] * right[1], left[0] * right[1] + left[1] * right[0])


def block_table(pair):
    cosine, sine_part = pair
    return jnp.stack([jnp.stack([cosine, -sine_part]), jnp.stack([sine_part, cosine])])


def product_of(left, right):
    return jnp.stack(
        [left[0] * right[0] - left[1] * right[1], left[0] * right[1] + left[1] * right[0]]
    )


def conj_product(left, right):
    return jnp.stack(
        [left[0] * right[0] + left[1] * right[1], left[0] * right[1] - left[1] * right[0]]
    )


def joined(left, right):
    return jnp.concatenate([left, right], axis=-1)


def factor(total):
    chosen = 1
    for candidate in range(1, total + 1):
        if candidate * candidate <= total and total % candidate == 0:
            chosen = candidate
    return chosen


def leading_section(values, seq_size):
    cosine, sine_part = angles(index_ramp(2 * seq_size), index_ramp(seq_size), 2 * seq_size, -1.0)
    table = jnp.stack([cosine, sine_part])
    return jnp.einsum("rkp,pmc->rkmc", table, values, precision=HIGHEST)


def trailing_section(values, seq_size, period):
    cosine, sine_part = angles(index_ramp(seq_size), index_ramp(2 * seq_size), 2 * seq_size, 1.0)
    table = jnp.stack([cosine, -sine_part]) * (1.0 / period)
    return jnp.einsum("rpk,rkmc->pmc", table, values, precision=HIGHEST)


def inner_forward(values, freq_keys, period):
    lead_size, row_count, chan_count = values.shape[1:]
    outer_size = factor(row_count)
    inner_size = row_count // outer_size
    values = values.reshape(2, lead_size, outer_size, inner_size, chan_count)
    first_twiddle = angles(freq_keys, index_ramp(row_count), period, -1.0)
    first_twiddle = tuple(
        (part.reshape(lead_size, outer_size, inner_size) for part in first_twiddle)
    )
    outer_dft = angles(index_ramp(outer_size), index_ramp(outer_size), outer_size, -1.0)
    outer_table = times_table(
        tuple((part[None, :, :, None] for part in outer_dft)),
        tuple((part[:, None, :, :] for part in first_twiddle)),
    )
    values = jnp.einsum("rsjxab,sjabc->rjxbc", block_table(outer_table), values, precision=HIGHEST)
    second_twiddle = angles(index_ramp(outer_size), index_ramp(inner_size), row_count, -1.0)
    inner_dft = angles(index_ramp(inner_size), index_ramp(inner_size), inner_size, -1.0)
    inner_table = times_table(
        tuple((part[None, :, :] for part in inner_dft)),
        tuple((part[:, None, :] for part in second_twiddle)),
    )
    return jnp.einsum("rsxyb,sjxbc->rjxyc", block_table(inner_table), values, precision=HIGHEST)


def inner_inverse(values, freq_keys, period):
    lead_size, outer_size, inner_size, chan_count = values.shape[1:]
    row_count = outer_size * inner_size
    second_twiddle = angles(index_ramp(outer_size), index_ramp(inner_size), row_count, 1.0)
    inner_dft = angles(index_ramp(inner_size), index_ramp(inner_size), inner_size, 1.0)
    inner_table = times_table(
        tuple((part[:, :, None] for part in second_twiddle)),
        tuple((part[None, :, :] for part in inner_dft)),
    )
    values = jnp.einsum("rsxby,sjxyc->rjxbc", block_table(inner_table), values, precision=HIGHEST)
    first_twiddle = angles(freq_keys, index_ramp(row_count), period, 1.0)
    first_twiddle = tuple(
        (part.reshape(lead_size, outer_size, inner_size) for part in first_twiddle)
    )
    outer_dft = angles(index_ramp(outer_size), index_ramp(outer_size), outer_size, 1.0)
    outer_table = times_table(
        tuple((part[:, :, :, None] for part in first_twiddle)),
        tuple((part[None, :, None, :] for part in outer_dft)),
    )
    values = jnp.einsum("rsjabx,sjxbc->rjabc", block_table(outer_table), values, precision=HIGHEST)
    return values.reshape(2, lead_size, row_count, chan_count)


def forward_local(signal_part, seq_size):
    seq_length, chan_count = signal_part.shape
    row_count = seq_length // seq_size
    values = leading_section(signal_part.reshape(seq_size, row_count, chan_count), seq_size)
    return inner_forward(values, index_ramp(2 * seq_size), 2 * seq_length)


def inverse_local(values, seq_size):
    lead_size, outer_size, inner_size, chan_count = values.shape[1:]
    row_count = outer_size * inner_size
    period = 2 * seq_size * row_count
    values = inner_inverse(values, index_ramp(2 * seq_size), period)
    return trailing_section(values, seq_size, period).reshape(seq_size * row_count, chan_count)


def filter_times_pair(spec_filter, spec_pair):
    shape_pair = spec_pair.shape
    width = spec_filter.shape[-1]
    pair_view = spec_pair.reshape(shape_pair[:-1] + (2, width))
    filter_view = spec_filter[..., None, :]
    return product_of(filter_view, pair_view).reshape(shape_pair)


def staged_device(fwd_q, fwd_k, fwd_v, bwd_q, bwd_k, bwd_v, bwd_grad, filters, skip):
    row_count, chan_width = fwd_q.shape
    seq_size = lax.axis_size("seq")
    grad_scale = 1.0 / math.sqrt(row_count * seq_size)
    source = (widened(fwd_k) * widened(fwd_v)).astype(jnp.bfloat16)
    second_source = (widened(bwd_k) * widened(bwd_v)).astype(jnp.bfloat16)
    upstream = (widened(bwd_grad) * widened(bwd_q)).astype(jnp.bfloat16)
    skip_gain = widened(skip)
    filters_all = lax.all_gather(filters, "chan", axis=1, tiled=True)
    narrow = chan_width // seq_size
    local_first, local_second = (
        lax.all_to_all(source, "seq", split_axis=1, concat_axis=0, tiled=True),
        lax.all_to_all(second_source, "seq", split_axis=1, concat_axis=0, tiled=True),
    )
    local_filter = lax.all_to_all(filters_all, "seq", split_axis=1, concat_axis=0, tiled=True)
    local_up = lax.all_to_all(upstream, "seq", split_axis=1, concat_axis=0, tiled=True)
    spec_sources = forward_local(
        widened(jnp.concatenate([local_first, local_second], axis=1)), seq_size
    )
    spec_filter = forward_local(local_filter, seq_size)
    conv_local = inverse_local(filter_times_pair(spec_filter, spec_sources), seq_size)
    conv_first, conv_second = (
        lax.all_to_all(conv_local[:, :narrow], "seq", split_axis=0, concat_axis=1, tiled=True),
        lax.all_to_all(conv_local[:, narrow:], "seq", split_axis=0, concat_axis=1, tiled=True),
    )
    spec_up = forward_local(widened(local_up), seq_size)
    spec_second = spec_sources[..., narrow:]
    back_local = inverse_local(
        joined(conj_product(spec_filter, spec_up), conj_product(spec_second, spec_up)), seq_size
    )
    through_conv, filter_terms = (
        lax.all_to_all(back_local[:, :narrow], "seq", split_axis=0, concat_axis=1, tiled=True),
        lax.all_to_all(
            back_local[:, narrow:] * grad_scale, "seq", split_axis=0, concat_axis=1, tiled=True
        ),
    )
    grad_filter = lax.psum_scatter(filter_terms, "chan", scatter_dimension=1, tiled=True)
    source_wide = widened(source)
    second_wide = widened(second_source)
    upstream_wide = widened(upstream)
    mixed = conv_first + skip_gain * source_wide
    output = (widened(fwd_q) * mixed).astype(jnp.bfloat16)
    mixed_two = conv_second + skip_gain * second_wide
    grad_query = (widened(bwd_grad) * mixed_two).astype(jnp.bfloat16)
    through = through_conv + skip_gain * upstream_wide
    grad_key = (through * widened(bwd_v)).astype(jnp.bfloat16)
    grad_value = (through * widened(bwd_k)).astype(jnp.bfloat16)
    grad_skip = lax.psum(jnp.sum(upstream_wide * second_wide, axis=0) * grad_scale, "seq")
    return (output, grad_query, grad_key, grad_value, grad_filter, grad_skip)


LANES = 128
TABLE_BUDGET = 32 * 1024 * 1024
BF = jnp.bfloat16
F32 = jnp.float32


def power_of_two(value):
    return value & (value - 1) == 0


class Plan:
    def __init__(self, rows, width, filt, seq, chan):
        self.rows, self.width, self.filt, self.seq, self.chan = rows, width, filt, seq, chan
        self.length = rows * seq
        self.strip = filt // seq
        self.groups = LANES // self.strip if self.strip else 0
        self.packed = rows // self.groups if self.groups else 0
        self.tiles = self.length // LANES

    def fits(self):
        return (
            self.width == self.seq * LANES
            and self.filt * self.chan == self.width
            and self.strip * self.chan == LANES
            and self.groups * self.strip == LANES
            and self.rows % LANES == 0
            and self.rows % self.tiles == 0
            and self.packed % 16 == 0
            and (3 * self.rows) % self.packed == 0
            and power_of_two(self.seq)
            and power_of_two(self.chan)
            and 2 * self.length * self.length * 2 <= TABLE_BUDGET
        )


def lane_index(rows):
    return lax.broadcasted_iota(jnp.int32, (rows, LANES), 1)


def unit_circle(steps, period):
    phase = (steps % period).astype(F32) * (2.0 * math.pi / period)
    return jnp.cos(phase), -jnp.sin(phase)


def cmul(left, right):
    return (left[0] * right[0] - left[1] * right[1], left[0] * right[1] + left[1] * right[0])


def table_kernel(plan, pos, fwd_ref, inv_ref, base_ref, turned_ref):
    length, rows = plan.length, plan.rows
    period = 4 * length
    me = pos[0]
    tile = pl.program_id(0)
    fine = 16
    column = lax.broadcasted_iota(jnp.int32, (1, length), 1)
    block = column // rows
    time = (block ^ me) * rows + column % rows

    @pl.when(tile == 0)
    def _():
        coarse_k = lax.broadcasted_iota(jnp.int32, (LANES // fine, length), 0) * (4 * fine)
        coarse = unit_circle(coarse_k * time, period)
        fine_k = lax.broadcasted_iota(jnp.int32, (fine, length), 0) * 4 + 1
        close = unit_circle(fine_k * time, period)
        for a in range(LANES // fine):
            real, imag = cmul((coarse[0][a : a + 1], coarse[1][a : a + 1]), close)
            base_ref[0, a * fine : (a + 1) * fine, :] = real
            base_ref[1, a * fine : (a + 1) * fine, :] = imag
        key = 4 * lax.broadcasted_iota(jnp.int32, (1, LANES), 1) + 1
        inner = unit_circle(
            lax.broadcasted_iota(jnp.int32, (rows, LANES), 0) * (4 * lane_index(rows) + 1), period
        )
        for d in range(plan.seq):
            start = unit_circle(key * ((me ^ d) * rows), period)
            real, imag = cmul(start, inner)
            turned_ref[0, d * rows : (d + 1) * rows, :] = real
            turned_ref[1, d * rows : (d + 1) * rows, :] = imag

    step = unit_circle(tile * time, plan.tiles)
    real, imag = cmul(step, (base_ref[0], base_ref[1]))
    fwd_ref[0, :LANES, :] = real.astype(BF)
    fwd_ref[0, LANES:, :] = imag.astype(BF)
    turn = unit_circle(tile * lax.broadcasted_iota(jnp.int32, (rows, LANES), 0), plan.tiles)
    turn = (turn[0] * (1.0 / length), turn[1] * (1.0 / length))
    for d in range(plan.seq):
        part = slice(d * rows, (d + 1) * rows)
        real, imag = cmul(turn, (turned_ref[0, part, :], turned_ref[1, part, :]))
        inv_ref[0, part, :LANES] = real.astype(BF)
        inv_ref[0, part, LANES:] = imag.astype(BF)


def make_tables(plan, pos):
    length, tiles = plan.length, plan.tiles
    return pl.pallas_call(
        lambda *refs: table_kernel(plan, *refs),
        grid=(tiles,),
        in_specs=[pl.BlockSpec(memory_space=pltpu.SMEM)],
        out_specs=[
            pl.BlockSpec((1, 2 * LANES, length), lambda i: (i, 0, 0)),
            pl.BlockSpec((1, length, 2 * LANES), lambda i: (i, 0, 0)),
        ],
        out_shape=[
            jax.ShapeDtypeStruct((tiles, 2 * LANES, length), BF),
            jax.ShapeDtypeStruct((tiles, length, 2 * LANES), BF),
        ],
        scratch_shapes=[
            pltpu.VMEM((2, LANES, length), F32),
            pltpu.VMEM((2, length, LANES), F32),
        ],
        cost_estimate=pl.CostEstimate(flops=400_000_000, bytes_accessed=8 * length * length, transcendentals=0),
        name="tables",
    )(pos)


def strip_place(plan, index, group):
    offset = group * plan.filt + index * plan.strip
    start = pl.multiple_of(offset // LANES * LANES, LANES)
    return start, offset % LANES


def pack_kernel(plan, pos, fk, fv, bk, bv, bg, bq, filters, *rest):
    outs, gated = rest[:-1], rest[-1]
    rows, strip, packed = plan.rows, plan.strip, plan.packed
    me, zi = pos[0], pos[1]
    for a, (left, right) in enumerate(((fk, fv), (bk, bv), (bg, bq))):
        gated[a * rows : (a + 1) * rows, :] = left[...].astype(F32) * right[...].astype(F32)
    lane = lane_index(3 * rows) // strip
    small = lane_index(packed) // strip
    for d in range(plan.seq):
        dest = me ^ d
        total = None
        for e in range(plan.chan):
            start, rest_of = strip_place(plan, dest, zi ^ e)
            turned = pltpu.roll(
                gated[:, pl.ds(start, LANES)], (e * strip + LANES - rest_of) % LANES, 1
            )
            total = turned if e == 0 else jnp.where(lane == e, turned, total)
        outs[d][: 3 * rows, :] = total.astype(BF)
        start, rest_of = strip_place(plan, dest, 0)
        total = None
        for g in range(plan.groups):
            turned = pltpu.roll(
                filters[g * packed : (g + 1) * packed, pl.ds(start, LANES)],
                (g * strip + LANES - rest_of) % LANES,
                1,
            )
            total = turned if g == 0 else jnp.where(small == g, turned, total)
        outs[d][3 * rows :, :] = total.astype(BF)


def pack_messages(plan, pos, arrays, filters):
    height = 3 * plan.rows + plan.packed
    vmem = pl.BlockSpec(memory_space=pltpu.VMEM)
    return pl.pallas_call(
        lambda *refs: pack_kernel(plan, *refs),
        in_specs=[pl.BlockSpec(memory_space=pltpu.SMEM)] + [vmem] * 7,
        out_specs=[vmem] * plan.seq,
        out_shape=[jax.ShapeDtypeStruct((height, LANES), BF)] * plan.seq,
        scratch_shapes=[pltpu.VMEM((3 * plan.rows, plan.width), F32)],
        name="pack",
    )(pos, *arrays, filters)


def collect_kernel(packed, *refs):
    for d, ref in enumerate(refs[:-1]):
        refs[-1][d * packed : (d + 1) * packed, :] = ref[...]


def collect_filters(plan, messages):
    packed = plan.packed
    row = 3 * plan.rows // packed
    return pl.pallas_call(
        lambda *refs: collect_kernel(packed, *refs),
        grid=(1,),
        in_specs=[pl.BlockSpec((packed, LANES), lambda i: (row, 0))] * plan.seq,
        out_specs=pl.BlockSpec((plan.seq * packed, LANES), lambda i: (0, 0)),
        out_shape=jax.ShapeDtypeStruct((plan.seq * packed, LANES), BF),
        name="collect",
    )(*messages)


def matmul(left, right):
    return lax.dot_general(left, right, (((1,), (0,)), ((), ())), preferred_element_type=F32)


def early_kernel(plan, fwd, inv, *refs):
    seq, rows, strip, packed = plan.seq, plan.rows, plan.strip, plan.packed
    messages, refs = refs[:seq], refs[seq:]
    spec_ref, strips, dots_ref, wide, total = (
        refs[0], refs[1 : 1 + plan.chan], refs[1 + plan.chan], refs[2 + plan.chan], refs[3 + plan.chan]
    )
    tile = pl.program_id(0)

    @pl.when(tile == 0)
    def _():
        dots = jnp.zeros((1, LANES), F32)
        for d in range(seq):
            second = messages[d][rows : 2 * rows, :]
            upstream = messages[d][2 * rows : 3 * rows, :]
            wide[d * rows : (d + 1) * rows, :LANES] = second
            wide[d * rows : (d + 1) * rows, LANES:] = upstream
            dots = dots + jnp.sum(second.astype(F32) * upstream.astype(F32), axis=0, keepdims=True)
        dots_ref[...] = jnp.broadcast_to(dots, (8, LANES))

    spec = matmul(fwd[0], wide[...])
    spec_ref[0] = spec.astype(BF)
    s_r, s_i = spec[:LANES, :LANES], spec[LANES:, :LANES]
    u_r, u_i = spec[:LANES, LANES:], spec[LANES:, LANES:]
    product = jnp.concatenate([s_r * u_r + s_i * u_i, s_r * u_i - s_i * u_r], axis=0).astype(BF)
    part = matmul(inv[0], product)

    @pl.when(tile == 0)
    def _():
        total[...] = part

    @pl.when(tile > 0)
    def _():
        total[...] += part

    @pl.when(tile == plan.tiles - 1)
    def _():
        lane = lane_index(packed) // strip
        for e in range(plan.chan):
            for d in range(seq):
                out = None
                for g in range(plan.groups):
                    top = d * rows + g * packed
                    turned = pltpu.roll(total[top : top + packed, :], (g - e) * strip % LANES, 1)
                    out = turned if g == 0 else jnp.where(lane == g, turned, out)
                strips[e][d * packed : (d + 1) * packed, :] = out.astype(BF)


def early_transforms(plan, tables, messages):
    length, seq, rows = plan.length, plan.seq, plan.rows
    height = 3 * rows + plan.packed
    strips = seq * plan.packed
    fixed = lambda i: (0, 0)
    return pl.pallas_call(
        lambda *refs: early_kernel(plan, *refs),
        grid=(plan.tiles,),
        in_specs=[
            pl.BlockSpec((1, 2 * LANES, length), lambda i: (i, 0, 0)),
            pl.BlockSpec((1, length, 2 * LANES), lambda i: (i, 0, 0)),
        ]
        + [pl.BlockSpec((height, LANES), fixed)] * seq,
        out_specs=[pl.BlockSpec((1, 2 * LANES, 2 * LANES), lambda i: (i, 0, 0))]
        + [pl.BlockSpec((strips, LANES), fixed)] * plan.chan
        + [pl.BlockSpec((8, LANES), fixed)],
        out_shape=[jax.ShapeDtypeStruct((plan.tiles, 2 * LANES, 2 * LANES), BF)]
        + [jax.ShapeDtypeStruct((strips, LANES), BF)] * plan.chan
        + [jax.ShapeDtypeStruct((8, LANES), F32)],
        scratch_shapes=[
            pltpu.VMEM((length, 2 * LANES), BF),
            pltpu.VMEM((length, LANES), F32),
        ],
        cost_estimate=pl.CostEstimate(flops=1_500_000_000, bytes_accessed=8 * length * length, transcendentals=0),
        name="early",
    )(*tables, *messages)


def late_kernel(plan, fwd, inv, spec_ref, dots_ref, *refs):
    seq, chan, rows, strip, packed = plan.seq, plan.chan, plan.rows, plan.strip, plan.packed
    messages, refs = refs[:seq], refs[seq:]
    pieces, refs = refs[:chan], refs[chan:]
    strips, refs = refs[:chan], refs[chan:]
    outs, (wide, total) = refs[:seq], refs[seq:]
    tile = pl.program_id(0)

    @pl.when(tile == 0)
    def _():
        lane = lane_index(packed) // strip
        for d in range(seq):
            wide[d * rows : (d + 1) * rows, :LANES] = messages[d][...]
            part = slice(d * packed, (d + 1) * packed)
            for g in range(plan.groups):
                out = None
                for e in range(chan):
                    turned = pltpu.roll(pieces[e][part, :].astype(F32), (e - g) * strip % LANES, 1)
                    out = turned if e == 0 else jnp.where(lane == e, turned, out)
                top = d * rows + g * packed
                wide[top : top + packed, LANES:] = out.astype(BF)

    spec = matmul(fwd[0], wide[...])
    f_r, f_i = spec[:LANES, :LANES], spec[LANES:, :LANES]
    k_r, k_i = spec[:LANES, LANES:], spec[LANES:, LANES:]
    saved = spec_ref[0].astype(F32)
    s_r, s_i = saved[:LANES, :LANES], saved[LANES:, :LANES]
    u_r, u_i = saved[:LANES, LANES:], saved[LANES:, LANES:]
    top = jnp.concatenate([k_r * f_r - k_i * f_i, k_r * s_r - k_i * s_i, k_r * u_r + k_i * u_i], axis=1)
    low = jnp.concatenate([k_r * f_i + k_i * f_r, k_r * s_i + k_i * s_r, k_r * u_i - k_i * u_r], axis=1)
    part = matmul(inv[0], jnp.concatenate([top, low], axis=0).astype(BF))

    @pl.when(tile == 0)
    def _():
        total[...] = part

    @pl.when(tile > 0)
    def _():
        total[...] += part

    @pl.when(tile == plan.tiles - 1)
    def _():
        dots = dots_ref[0:1, :]
        high = dots.astype(BF).astype(F32)
        middle = (dots - high).astype(BF).astype(F32)
        low = dots - high - middle
        row = lax.broadcasted_iota(jnp.int32, (16, LANES), 0)
        tail = jnp.where(row == 0, high, jnp.where(row == 1, middle, jnp.where(row == 2, low, 0.0)))
        for d in range(seq):
            for a in range(3):
                outs[d][a * rows : (a + 1) * rows, :] = total[
                    d * rows : (d + 1) * rows, a * LANES : (a + 1) * LANES
                ].astype(BF)
            part = slice(d * packed, (d + 1) * packed)
            summed = strips[0][part, :].astype(F32)
            for e in range(1, chan):
                summed = summed + strips[e][part, :].astype(F32)
            outs[d][3 * rows : 3 * rows + packed, :] = summed.astype(BF)
            outs[d][3 * rows + packed :, :] = tail.astype(BF)


def late_transforms(plan, tables, spec, dots, messages, pieces, strips):
    length, seq, rows, packed = plan.length, plan.seq, plan.rows, plan.packed
    height = 3 * rows + packed + 16
    fixed = lambda i: (0, 0)
    return pl.pallas_call(
        lambda *refs: late_kernel(plan, *refs),
        grid=(plan.tiles,),
        in_specs=[
            pl.BlockSpec((1, 2 * LANES, length), lambda i: (i, 0, 0)),
            pl.BlockSpec((1, length, 2 * LANES), lambda i: (i, 0, 0)),
            pl.BlockSpec((1, 2 * LANES, 2 * LANES), lambda i: (i, 0, 0)),
            pl.BlockSpec((8, LANES), fixed),
        ]
        + [pl.BlockSpec((rows, LANES), fixed)] * seq
        + [pl.BlockSpec((seq * packed, LANES), fixed)] * (2 * plan.chan),
        out_specs=[pl.BlockSpec((height, LANES), fixed)] * seq,
        out_shape=[jax.ShapeDtypeStruct((height, LANES), BF)] * seq,
        scratch_shapes=[
            pltpu.VMEM((length, 2 * LANES), BF),
            pltpu.VMEM((length, 3 * LANES), F32),
        ],
        cost_estimate=pl.CostEstimate(flops=3_000_000_000, bytes_accessed=8 * length * length, transcendentals=0),
        name="late",
    )(*tables, spec, dots, *messages, *pieces, *strips)


def finish_kernel(plan, scale, pos, fq, fk, fv, bq, bk, bv, bg, skip, *refs):
    seq, rows, strip, packed = plan.seq, plan.rows, plan.strip, plan.packed
    messages, refs = refs[:seq], refs[seq:]
    out, g_query, g_key, g_value, g_filter, g_skip, spread, skips = refs
    me, zi = pos[0], pos[1]
    lane = lane_index(3 * rows) // strip
    small = lane_index(packed) // strip
    for d in range(seq):
        source = me ^ d
        ready = messages[d][: 3 * rows, :].astype(F32)
        tail = messages[d][3 * rows + packed :, :].astype(F32)
        dots = jnp.broadcast_to(jnp.sum(tail, axis=0, keepdims=True) * scale, (8, LANES))
        for e in range(plan.chan):
            start, rest_of = strip_place(plan, source, zi ^ e)
            turn = (rest_of + LANES - e * strip) % LANES
            here = lane == rest_of // strip
            spread[:, pl.ds(start, LANES)] = jnp.where(
                here, pltpu.roll(ready, turn, 1), spread[:, pl.ds(start, LANES)]
            )
            skips[:, pl.ds(start, LANES)] = jnp.where(
                here[:8], pltpu.roll(dots, turn, 1), skips[:, pl.ds(start, LANES)]
            )
        terms = messages[d][3 * rows : 3 * rows + packed, :].astype(F32) * scale
        start, rest_of = strip_place(plan, source, 0)
        for g in range(plan.groups):
            part = slice(g * packed, (g + 1) * packed)
            g_filter[part, pl.ds(start, LANES)] = jnp.where(
                small == rest_of // strip,
                pltpu.roll(terms, (rest_of + LANES - g * strip) % LANES, 1),
                g_filter[part, pl.ds(start, LANES)],
            )
    g_skip[...] = skips[0:1, :]
    gain = skip[...]

    def gated(left, right):
        return (left[...].astype(F32) * right[...].astype(F32)).astype(BF).astype(F32)

    out[...] = (fq[...].astype(F32) * (spread[:rows, :] + gain * gated(fk, fv))).astype(BF)
    mixed = spread[rows : 2 * rows, :] + gain * gated(bk, bv)
    g_query[...] = (bg[...].astype(F32) * mixed).astype(BF)
    through = spread[2 * rows :, :] + gain * gated(bg, bq)
    g_key[...] = (through * bv[...].astype(F32)).astype(BF)
    g_value[...] = (through * bk[...].astype(F32)).astype(BF)


def finish(plan, scale, pos, arrays, skip, messages):
    rows, width = plan.rows, plan.width
    vmem = pl.BlockSpec(memory_space=pltpu.VMEM)
    return pl.pallas_call(
        lambda *refs: finish_kernel(plan, scale, *refs),
        in_specs=[pl.BlockSpec(memory_space=pltpu.SMEM)] + [vmem] * (8 + plan.seq),
        out_specs=[vmem] * 6,
        out_shape=[jax.ShapeDtypeStruct((rows, width), BF)] * 4
        + [jax.ShapeDtypeStruct((rows, plan.filt), F32), jax.ShapeDtypeStruct((1, width), F32)],
        scratch_shapes=[pltpu.VMEM((3 * rows, width), F32), pltpu.VMEM((8, width), F32)],
        name="finish",
    )(pos, *arrays, skip, *messages)


def swap(value, axis, size, distance):
    return lax.ppermute(value, axis, [(i, i ^ distance) for i in range(size)])


def exchange(values, axis, order):
    size = len(values)
    got = {0: values[0]}
    for d in order:
        got[d] = swap(values[d], axis, size, d)
    return [got[d] for d in range(size)]


def dense_device(plan, fwd_q, fwd_k, fwd_v, bwd_q, bwd_k, bwd_v, bwd_grad, filters, skip):
    pos = jnp.stack([lax.axis_index("seq"), lax.axis_index("chan")]).astype(jnp.int32)
    scale = 1.0 / math.sqrt(plan.length)
    far_first = list(range(2, plan.seq)) + [1]
    messages = pack_messages(plan, pos, (fwd_k, fwd_v, bwd_k, bwd_v, bwd_grad, bwd_q), filters)
    tables = make_tables(plan, pos)
    messages = exchange(messages, "seq", far_first)
    mine = collect_filters(plan, messages)
    pieces = exchange([mine] * plan.chan, "chan", range(1, plan.chan))
    spec, *rest = early_transforms(plan, tables, messages)
    strips, dots = rest[:-1], rest[-1]
    strips = exchange(strips, "chan", range(1, plan.chan))
    results = late_transforms(plan, tables, spec, dots, messages, pieces, strips)
    results = exchange(results, "seq", far_first)
    arrays = (fwd_q, fwd_k, fwd_v, bwd_q, bwd_k, bwd_v, bwd_grad)
    out, g_query, g_key, g_value, g_filter, g_skip = finish(
        plan, scale, pos, arrays, skip.reshape(1, -1), results
    )
    return out, g_query, g_key, g_value, g_filter, g_skip.reshape(-1)


def per_device(*arrays):
    rows, width = arrays[0].shape
    plan = Plan(rows, width, arrays[7].shape[1], lax.axis_size("seq"), lax.axis_size("chan"))
    if plan.fits():
        return dense_device(plan, *arrays)
    return staged_device(*arrays)


def solution(mesh):
    return jax.shard_map(
        per_device,
        mesh=mesh,
        in_specs=(
            P("seq", "chan"),
            P("seq", "chan"),
            P("seq", "chan"),
            P("seq", "chan"),
            P("seq", "chan"),
            P("seq", "chan"),
            P("seq", "chan"),
            P("seq", "chan"),
            P("chan"),
        ),
        out_specs=(
            P("seq", "chan"),
            P("seq", "chan"),
            P("seq", "chan"),
            P("seq", "chan"),
            P("seq", "chan"),
            P("chan"),
        ),
        check_vma=False,
    )
```

```python
import math

import jax
import jax.numpy as jnp
from jax import lax
from jax.experimental import pallas as pl
from jax.experimental.pallas import tpu as pltpu
from jax.sharding import PartitionSpec as P


HIGHEST = lax.Precision.HIGHEST


def index_ramp(total):
    return jnp.arange(total, dtype=jnp.int32)


def widened(values):
    return values.astype(jnp.float32)


def angles(out_index, in_index, period, sign):
    phase_steps = out_index[:, None] * in_index[None, :] % period
    phase = phase_steps.astype(jnp.float32) * (sign * 2.0 * math.pi / period)
    return (jnp.cos(phase), jnp.sin(phase))


def times_table(left, right):
    return (left[0] * right[0] - left[1] * right[1], left[0] * right[1] + left[1] * right[0])


def block_table(pair):
    cosine, sine_part = pair
    return jnp.stack([jnp.stack([cosine, -sine_part]), jnp.stack([sine_part, cosine])])


def product_of(left, right):
    return jnp.stack(
        [left[0] * right[0] - left[1] * right[1], left[0] * right[1] + left[1] * right[0]]
    )


def conj_product(left, right):
    return jnp.stack(
        [left[0] * right[0] + left[1] * right[1], left[0] * right[1] - left[1] * right[0]]
    )


def joined(left, right):
    return jnp.concatenate([left, right], axis=-1)


def factor(total):
    chosen = 1
    for candidate in range(1, total + 1):
        if candidate * candidate <= total and total % candidate == 0:
            chosen = candidate
    return chosen


def leading_section(values, seq_size):
    cosine, sine_part = angles(index_ramp(2 * seq_size), index_ramp(seq_size), 2 * seq_size, -1.0)
    table = jnp.stack([cosine, sine_part])
    return jnp.einsum("rkp,pmc->rkmc", table, values, precision=HIGHEST)


def trailing_section(values, seq_size, period):
    cosine, sine_part = angles(index_ramp(seq_size), index_ramp(2 * seq_size), 2 * seq_size, 1.0)
    table = jnp.stack([cosine, -sine_part]) * (1.0 / period)
    return jnp.einsum("rpk,rkmc->pmc", table, values, precision=HIGHEST)


def inner_forward(values, freq_keys, period):
    lead_size, row_count, chan_count = values.shape[1:]
    outer_size = factor(row_count)
    inner_size = row_count // outer_size
    values = values.reshape(2, lead_size, outer_size, inner_size, chan_count)
    first_twiddle = angles(freq_keys, index_ramp(row_count), period, -1.0)
    first_twiddle = tuple(
        (part.reshape(lead_size, outer_size, inner_size) for part in first_twiddle)
    )
    outer_dft = angles(index_ramp(outer_size), index_ramp(outer_size), outer_size, -1.0)
    outer_table = times_table(
        tuple((part[None, :, :, None] for part in outer_dft)),
        tuple((part[:, None, :, :] for part in first_twiddle)),
    )
    values = jnp.einsum("rsjxab,sjabc->rjxbc", block_table(outer_table), values, precision=HIGHEST)
    second_twiddle = angles(index_ramp(outer_size), index_ramp(inner_size), row_count, -1.0)
    inner_dft = angles(index_ramp(inner_size), index_ramp(inner_size), inner_size, -1.0)
    inner_table = times_table(
        tuple((part[None, :, :] for part in inner_dft)),
        tuple((part[:, None, :] for part in second_twiddle)),
    )
    return jnp.einsum("rsxyb,sjxbc->rjxyc", block_table(inner_table), values, precision=HIGHEST)


def inner_inverse(values, freq_keys, period):
    lead_size, outer_size, inner_size, chan_count = values.shape[1:]
    row_count = outer_size * inner_size
    second_twiddle = angles(index_ramp(outer_size), index_ramp(inner_size), row_count, 1.0)
    inner_dft = angles(index_ramp(inner_size), index_ramp(inner_size), inner_size, 1.0)
    inner_table = times_table(
        tuple((part[:, :, None] for part in second_twiddle)),
        tuple((part[None, :, :] for part in inner_dft)),
    )
    values = jnp.einsum("rsxby,sjxyc->rjxbc", block_table(inner_table), values, precision=HIGHEST)
    first_twiddle = angles(freq_keys, index_ramp(row_count), period, 1.0)
    first_twiddle = tuple(
        (part.reshape(lead_size, outer_size, inner_size) for part in first_twiddle)
    )
    outer_dft = angles(index_ramp(outer_size), index_ramp(outer_size), outer_size, 1.0)
    outer_table = times_table(
        tuple((part[:, :, :, None] for part in first_twiddle)),
        tuple((part[None, :, None, :] for part in outer_dft)),
    )
    values = jnp.einsum("rsjabx,sjxbc->rjabc", block_table(outer_table), values, precision=HIGHEST)
    return values.reshape(2, lead_size, row_count, chan_count)


def forward_local(signal_part, seq_size):
    seq_length, chan_count = signal_part.shape
    row_count = seq_length // seq_size
    values = leading_section(signal_part.reshape(seq_size, row_count, chan_count), seq_size)
    return inner_forward(values, index_ramp(2 * seq_size), 2 * seq_length)


def inverse_local(values, seq_size):
    lead_size, outer_size, inner_size, chan_count = values.shape[1:]
    row_count = outer_size * inner_size
    period = 2 * seq_size * row_count
    values = inner_inverse(values, index_ramp(2 * seq_size), period)
    return trailing_section(values, seq_size, period).reshape(seq_size * row_count, chan_count)


def filter_times_pair(spec_filter, spec_pair):
    shape_pair = spec_pair.shape
    width = spec_filter.shape[-1]
    pair_view = spec_pair.reshape(shape_pair[:-1] + (2, width))
    filter_view = spec_filter[..., None, :]
    return product_of(filter_view, pair_view).reshape(shape_pair)


def staged_device(fwd_q, fwd_k, fwd_v, bwd_q, bwd_k, bwd_v, bwd_grad, filters, skip):
    row_count, chan_width = fwd_q.shape
    seq_size = lax.axis_size("seq")
    grad_scale = 1.0 / math.sqrt(row_count * seq_size)
    source = (widened(fwd_k) * widened(fwd_v)).astype(jnp.bfloat16)
    second_source = (widened(bwd_k) * widened(bwd_v)).astype(jnp.bfloat16)
    upstream = (widened(bwd_grad) * widened(bwd_q)).astype(jnp.bfloat16)
    skip_gain = widened(skip)
    filters_all = lax.all_gather(filters, "chan", axis=1, tiled=True)
    narrow = chan_width // seq_size
    local_first, local_second = (
        lax.all_to_all(source, "seq", split_axis=1, concat_axis=0, tiled=True),
        lax.all_to_all(second_source, "seq", split_axis=1, concat_axis=0, tiled=True),
    )
    local_filter = lax.all_to_all(filters_all, "seq", split_axis=1, concat_axis=0, tiled=True)
    local_up = lax.all_to_all(upstream, "seq", split_axis=1, concat_axis=0, tiled=True)
    spec_sources = forward_local(
        widened(jnp.concatenate([local_first, local_second], axis=1)), seq_size
    )
    spec_filter = forward_local(local_filter, seq_size)
    conv_local = inverse_local(filter_times_pair(spec_filter, spec_sources), seq_size)
    conv_first, conv_second = (
        lax.all_to_all(conv_local[:, :narrow], "seq", split_axis=0, concat_axis=1, tiled=True),
        lax.all_to_all(conv_local[:, narrow:], "seq", split_axis=0, concat_axis=1, tiled=True),
    )
    spec_up = forward_local(widened(local_up), seq_size)
    spec_second = spec_sources[..., narrow:]
    back_local = inverse_local(
        joined(conj_product(spec_filter, spec_up), conj_product(spec_second, spec_up)), seq_size
    )
    through_conv, filter_terms = (
        lax.all_to_all(back_local[:, :narrow], "seq", split_axis=0, concat_axis=1, tiled=True),
        lax.all_to_all(
            back_local[:, narrow:] * grad_scale, "seq", split_axis=0, concat_axis=1, tiled=True
        ),
    )
    grad_filter = lax.psum_scatter(filter_terms, "chan", scatter_dimension=1, tiled=True)
    source_wide = widened(source)
    second_wide = widened(second_source)
    upstream_wide = widened(upstream)
    mixed = conv_first + skip_gain * source_wide
    output = (widened(fwd_q) * mixed).astype(jnp.bfloat16)
    mixed_two = conv_second + skip_gain * second_wide
    grad_query = (widened(bwd_grad) * mixed_two).astype(jnp.bfloat16)
    through = through_conv + skip_gain * upstream_wide
    grad_key = (through * widened(bwd_v)).astype(jnp.bfloat16)
    grad_value = (through * widened(bwd_k)).astype(jnp.bfloat16)
    grad_skip = lax.psum(jnp.sum(upstream_wide * second_wide, axis=0) * grad_scale, "seq")
    return (output, grad_query, grad_key, grad_value, grad_filter, grad_skip)


LANES = 128
TABLE_BUDGET = 32 * 1024 * 1024
BF = jnp.bfloat16
F32 = jnp.float32
VMEM_SPEC = pl.BlockSpec(memory_space=pltpu.VMEM)


def power_of_two(value):
    return value & (value - 1) == 0


class Plan:
    def __init__(self, rows, width, filt, seq, chan):
        self.rows, self.width, self.filt, self.seq, self.chan = rows, width, filt, seq, chan
        self.length = rows * seq
        self.strip = filt // seq
        self.groups = LANES // self.strip if self.strip else 0
        self.packed = rows // self.groups if self.groups else 0
        self.tiles = self.length // LANES

    def fits(self):
        return (
            self.width == self.seq * LANES
            and self.filt * self.chan == self.width
            and self.strip * self.chan == LANES
            and self.groups * self.strip == LANES
            and self.rows % LANES == 0
            and self.rows % self.tiles == 0
            and self.packed % 16 == 0
            and (3 * self.rows) % self.packed == 0
            and power_of_two(self.seq)
            and power_of_two(self.chan)
            and 2 * self.length * self.length * 2 <= TABLE_BUDGET
        )


def lane_index(rows):
    return lax.broadcasted_iota(jnp.int32, (rows, LANES), 1)


def unit_circle(steps, period):
    phase = (steps % period).astype(F32) * (2.0 * math.pi / period)
    return jnp.cos(phase), -jnp.sin(phase)


def cmul(left, right):
    return (left[0] * right[0] - left[1] * right[1], left[0] * right[1] + left[1] * right[0])


LIMIT = pltpu.CompilerParams(vmem_limit_bytes=20 * 1024 * 1024)


def table_kernel(plan, fwd_ref, inv_ref):
    length, rows, seq = plan.length, plan.rows, plan.seq
    period = 4 * length
    me = lax.axis_index("seq")
    fine = 16
    column = lax.broadcasted_iota(jnp.int32, (1, length), 1)
    time = ((column // rows) ^ me) * rows + column % rows
    coarse_k = lax.broadcasted_iota(jnp.int32, (LANES // fine, length), 0) * (4 * fine)
    coarse = unit_circle(coarse_k * time, period)
    close = unit_circle((lax.broadcasted_iota(jnp.int32, (fine, length), 0) * 4 + 1) * time, period)
    step = unit_circle(jnp.broadcast_to(time, (8, length)), plan.tiles)
    step = (step[0][0:1], step[1][0:1])
    for a in range(LANES // fine):
        part = slice(a * fine, (a + 1) * fine)
        value = cmul((coarse[0][a : a + 1], coarse[1][a : a + 1]), close)
        for tile in range(plan.tiles):
            top = tile * 2 * LANES + a * fine
            fwd_ref[top : top + fine, :] = value[0].astype(BF)
            fwd_ref[top + LANES : top + LANES + fine, :] = value[1].astype(BF)
            if tile + 1 < plan.tiles:
                value = cmul(value, step)
    key = 4 * lane_index(seq) + 1
    starts = unit_circle(key * ((lax.broadcasted_iota(jnp.int32, (seq, LANES), 0) ^ me) * rows), period)
    row = lax.broadcasted_iota(jnp.int32, (rows, LANES), 0)
    inner = unit_circle(row * (4 * lane_index(rows) + 1), period)
    inner = (inner[0] * (1.0 / length), inner[1] * (1.0 / length))
    turn = unit_circle(row, plan.tiles)
    for d in range(seq):
        part = slice(d * rows, (d + 1) * rows)
        value = cmul((starts[0][d : d + 1], starts[1][d : d + 1]), inner)
        for tile in range(plan.tiles):
            left = tile * 2 * LANES
            inv_ref[part, left : left + LANES] = value[0].astype(BF)
            inv_ref[part, left + LANES : left + 2 * LANES] = value[1].astype(BF)
            if tile + 1 < plan.tiles:
                value = cmul(value, turn)


def make_tables(plan):
    length = plan.length
    return pl.pallas_call(
        lambda *refs: table_kernel(plan, *refs),
        out_specs=[VMEM_SPEC] * 2,
        out_shape=[
            jax.ShapeDtypeStruct((2 * length, length), BF),
            jax.ShapeDtypeStruct((length, 2 * length), BF),
        ],
        cost_estimate=pl.CostEstimate(flops=400_000_000, bytes_accessed=8 * length * length, transcendentals=0),
        compiler_params=LIMIT,
        name="tables",
    )()


def strip_place(plan, index, group):
    offset = group * plan.filt + index * plan.strip
    start = pl.multiple_of(offset // LANES * LANES, LANES)
    return start, offset % LANES


def pack_kernel(plan, *refs):
    hbm, refs = refs[:7], refs[7:]
    outs, refs = refs[: plan.seq], refs[plan.seq :]
    local, (gated, sems) = refs[:7], refs[7:]
    rows, strip, packed = plan.rows, plan.strip, plan.packed
    me, zi = lax.axis_index("seq"), lax.axis_index("chan")
    copies = [pltpu.make_async_copy(hbm[n], local[n], sems.at[n]) for n in range(7)]
    for copy in copies:
        copy.start()
    lane = lane_index(rows) // strip
    small = lane_index(packed) // strip
    for a in range(3):
        copies[2 * a].wait()
        copies[2 * a + 1].wait()
        gated[a] = local[2 * a][...].astype(F32) * local[2 * a + 1][...].astype(F32)
        for d in range(plan.seq):
            total = None
            for e in range(plan.chan):
                start, rest_of = strip_place(plan, me ^ d, zi ^ e)
                turned = pltpu.roll(
                    gated[a, :, pl.ds(start, LANES)], (e * strip + LANES - rest_of) % LANES, 1
                )
                total = turned if e == 0 else jnp.where(lane == e, turned, total)
            outs[d][a * rows : (a + 1) * rows, :] = total.astype(BF)
    copies[6].wait()
    for d in range(plan.seq):
        start, rest_of = strip_place(plan, me ^ d, 0)
        total = None
        for g in range(plan.groups):
            turned = pltpu.roll(
                local[6][g * packed : (g + 1) * packed, pl.ds(start, LANES)],
                (g * strip + LANES - rest_of) % LANES,
                1,
            )
            total = turned if g == 0 else jnp.where(small == g, turned, total)
        outs[d][3 * rows :, :] = total.astype(BF)


def pack_messages(plan, arrays, filters):
    rows, width = plan.rows, plan.width
    height = 3 * rows + plan.packed
    return pl.pallas_call(
        lambda *refs: pack_kernel(plan, *refs),
        in_specs=[pl.BlockSpec(memory_space=pltpu.HBM)] * 7,
        out_specs=[VMEM_SPEC] * plan.seq,
        out_shape=[jax.ShapeDtypeStruct((height, LANES), BF)] * plan.seq,
        scratch_shapes=[pltpu.VMEM((rows, width), BF)] * 6
        + [
            pltpu.VMEM((rows, plan.filt), F32),
            pltpu.VMEM((3, rows, width), F32),
            pltpu.SemaphoreType.DMA((7,)),
        ],
        compiler_params=LIMIT,
        name="pack",
    )(*(pltpu.with_memory_space_constraint(a, pltpu.HBM) for a in (*arrays, filters)))


def collect_kernel(plan, *refs):
    packed = plan.packed
    for d, ref in enumerate(refs[:-1]):
        refs[-1][d * packed : (d + 1) * packed, :] = ref[3 * plan.rows :, :]


def collect_filters(plan, messages):
    return pl.pallas_call(
        lambda *refs: collect_kernel(plan, *refs),
        in_specs=[VMEM_SPEC] * plan.seq,
        out_specs=VMEM_SPEC,
        out_shape=jax.ShapeDtypeStruct((plan.seq * plan.packed, LANES), BF),
        compiler_params=LIMIT,
        name="collect",
    )(*messages)


def matmul(left, right):
    return lax.dot_general(left, right, (((1,), (0,)), ((), ())), preferred_element_type=F32)


def early_kernel(plan, fwd, inv, *refs):
    seq, rows, strip, packed = plan.seq, plan.rows, plan.strip, plan.packed
    messages, refs = refs[:seq], refs[seq:]
    spec_ref, strips, dots_ref, wide, products = (
        refs[0], refs[1 : 1 + plan.chan], refs[1 + plan.chan], refs[2 + plan.chan], refs[3 + plan.chan]
    )
    dots = jnp.zeros((1, LANES), F32)
    for d in range(seq):
        second = messages[d][rows : 2 * rows, :]
        upstream = messages[d][2 * rows : 3 * rows, :]
        wide[d * rows : (d + 1) * rows, :LANES] = second
        wide[d * rows : (d + 1) * rows, LANES:] = upstream
        dots = dots + jnp.sum(second.astype(F32) * upstream.astype(F32), axis=0, keepdims=True)
    dots_ref[...] = jnp.broadcast_to(dots, (8, LANES))
    for tile in range(plan.tiles):
        part = slice(tile * 2 * LANES, (tile + 1) * 2 * LANES)
        spec = matmul(fwd[part, :], wide[...])
        spec_ref[part, :] = spec.astype(BF)
        s_r, s_i = spec[:LANES, :LANES], spec[LANES:, :LANES]
        u_r, u_i = spec[:LANES, LANES:], spec[LANES:, LANES:]
        products[part, :] = jnp.concatenate(
            [s_r * u_r + s_i * u_i, s_r * u_i - s_i * u_r], axis=0
        ).astype(BF)
    lane = lane_index(packed) // strip
    span = 2
    for first in range(0, seq, span):
        total = matmul(inv[first * rows : (first + span) * rows, :], products[...])
        for d in range(first, first + span):
            for e in range(plan.chan):
                out = None
                for g in range(plan.groups):
                    top = (d - first) * rows + g * packed
                    turned = pltpu.roll(total[top : top + packed, :], (g - e) * strip % LANES, 1)
                    out = turned if g == 0 else jnp.where(lane == g, turned, out)
                strips[e][d * packed : (d + 1) * packed, :] = out.astype(BF)


def early_transforms(plan, tables, messages):
    length, seq = plan.length, plan.seq
    strips = seq * plan.packed
    return pl.pallas_call(
        lambda *refs: early_kernel(plan, *refs),
        in_specs=[VMEM_SPEC] * (2 + seq),
        out_specs=[VMEM_SPEC] * (2 + plan.chan),
        out_shape=[jax.ShapeDtypeStruct((2 * length, 2 * LANES), BF)]
        + [jax.ShapeDtypeStruct((strips, LANES), BF)] * plan.chan
        + [jax.ShapeDtypeStruct((8, LANES), F32)],
        scratch_shapes=[
            pltpu.VMEM((length, 2 * LANES), BF),
            pltpu.VMEM((2 * length, LANES), BF),
        ],
        cost_estimate=pl.CostEstimate(flops=1_500_000_000, bytes_accessed=8 * length * length, transcendentals=0),
        compiler_params=LIMIT,
        name="early",
    )(*tables, *messages)


def late_kernel(plan, fwd, inv, spec_ref, dots_ref, *refs):
    seq, chan, rows, strip, packed = plan.seq, plan.chan, plan.rows, plan.strip, plan.packed
    messages, refs = refs[:seq], refs[seq:]
    pieces, refs = refs[:chan], refs[chan:]
    outs, (wide, products) = refs[:seq], refs[seq:]
    lane = lane_index(packed) // strip
    for d in range(seq):
        wide[d * rows : (d + 1) * rows, :LANES] = messages[d][:rows, :]
        part = slice(d * packed, (d + 1) * packed)
        for g in range(plan.groups):
            out = None
            for e in range(chan):
                turned = pltpu.roll(pieces[e][part, :].astype(F32), (e - g) * strip % LANES, 1)
                out = turned if e == 0 else jnp.where(lane == e, turned, out)
            top = d * rows + g * packed
            wide[top : top + packed, LANES:] = out.astype(BF)
    for tile in range(plan.tiles):
        part = slice(tile * 2 * LANES, (tile + 1) * 2 * LANES)
        spec = matmul(fwd[part, :], wide[...])
        f_r, f_i = spec[:LANES, :LANES], spec[LANES:, :LANES]
        k_r, k_i = spec[:LANES, LANES:], spec[LANES:, LANES:]
        saved = spec_ref[part, :].astype(F32)
        s_r, s_i = saved[:LANES, :LANES], saved[LANES:, :LANES]
        u_r, u_i = saved[:LANES, LANES:], saved[LANES:, LANES:]
        for a, pair in enumerate((
            (k_r * f_r - k_i * f_i, k_r * f_i + k_i * f_r),
            (k_r * s_r - k_i * s_i, k_r * s_i + k_i * s_r),
            (k_r * u_r + k_i * u_i, k_r * u_i - k_i * u_r),
        )):
            products[part, a * LANES : (a + 1) * LANES] = jnp.concatenate(pair, axis=0).astype(BF)
    dots = dots_ref[0:1, :]
    high = dots.astype(BF).astype(F32)
    middle = (dots - high).astype(BF).astype(F32)
    low = dots - high - middle
    row = lax.broadcasted_iota(jnp.int32, (16, LANES), 0)
    tail = jnp.where(row == 0, high, jnp.where(row == 1, middle, jnp.where(row == 2, low, 0.0)))
    span = 2
    for first in range(0, seq, span):
        total = matmul(inv[first * rows : (first + span) * rows, :], products[...])
        for d in range(first, first + span):
            top = (d - first) * rows
            for a in range(3):
                outs[d][a * rows : (a + 1) * rows, :] = total[
                    top : top + rows, a * LANES : (a + 1) * LANES
                ].astype(BF)
            outs[d][3 * rows : 3 * rows + packed, :] = jnp.zeros((packed, LANES), BF)
            outs[d][3 * rows + packed :, :] = tail.astype(BF)


def late_transforms(plan, tables, spec, dots, messages, pieces):
    length, seq = plan.length, plan.seq
    height = 3 * plan.rows + plan.packed + 16
    return pl.pallas_call(
        lambda *refs: late_kernel(plan, *refs),
        in_specs=[VMEM_SPEC] * (4 + seq + plan.chan),
        out_specs=[VMEM_SPEC] * seq,
        out_shape=[jax.ShapeDtypeStruct((height, LANES), BF)] * seq,
        scratch_shapes=[
            pltpu.VMEM((length, 2 * LANES), BF),
            pltpu.VMEM((2 * length, 3 * LANES), BF),
        ],
        cost_estimate=pl.CostEstimate(flops=3_000_000_000, bytes_accessed=8 * length * length, transcendentals=0),
        compiler_params=LIMIT,
        name="late",
    )(*tables, spec, dots, *messages, *pieces)


def merge_kernel(plan, *refs):
    seq, chan, rows, packed = plan.seq, plan.chan, plan.rows, plan.packed
    strips, outs = refs[seq : seq + chan], refs[seq + chan :]
    for d in range(seq):
        part = slice(d * packed, (d + 1) * packed)
        summed = strips[0][part, :].astype(F32)
        for e in range(1, chan):
            summed = summed + strips[e][part, :].astype(F32)
        outs[d][3 * rows : 3 * rows + packed, :] = summed.astype(BF)


def merge_strips(plan, results, strips):
    seq = plan.seq
    return pl.pallas_call(
        lambda *refs: merge_kernel(plan, *refs),
        in_specs=[VMEM_SPEC] * (seq + plan.chan),
        out_specs=[VMEM_SPEC] * seq,
        out_shape=[jax.ShapeDtypeStruct(results[0].shape, BF)] * seq,
        input_output_aliases={d: d for d in range(seq)},
        compiler_params=LIMIT,
        name="merge",
    )(*results, *strips)


def finish_kernel(plan, scale, fq, fk, fv, bq, bk, bv, bg, skip, *refs):
    seq, rows, strip, packed = plan.seq, plan.rows, plan.strip, plan.packed
    messages, refs = refs[:seq], refs[seq:]
    out, g_query, g_key, g_value, g_filter, g_skip, spread, skips = refs
    me, zi = lax.axis_index("seq"), lax.axis_index("chan")
    lane = lane_index(3 * rows) // strip
    small = lane_index(packed) // strip
    for d in range(seq):
        source = me ^ d
        ready = messages[d][: 3 * rows, :].astype(F32)
        tail = messages[d][3 * rows + packed :, :].astype(F32)
        dots = jnp.broadcast_to(jnp.sum(tail, axis=0, keepdims=True) * scale, (8, LANES))
        for e in range(plan.chan):
            start, rest_of = strip_place(plan, source, zi ^ e)
            turn = (rest_of + LANES - e * strip) % LANES
            here = lane == rest_of // strip
            spread[:, pl.ds(start, LANES)] = jnp.where(
                here, pltpu.roll(ready, turn, 1), spread[:, pl.ds(start, LANES)]
            )
            skips[:, pl.ds(start, LANES)] = jnp.where(
                here[:8], pltpu.roll(dots, turn, 1), skips[:, pl.ds(start, LANES)]
            )
        terms = messages[d][3 * rows : 3 * rows + packed, :].astype(F32) * scale
        start, rest_of = strip_place(plan, source, 0)
        for g in range(plan.groups):
            part = slice(g * packed, (g + 1) * packed)
            g_filter[part, pl.ds(start, LANES)] = jnp.where(
                small == rest_of // strip,
                pltpu.roll(terms, (rest_of + LANES - g * strip) % LANES, 1),
                g_filter[part, pl.ds(start, LANES)],
            )
    g_skip[...] = skips[0:1, :]
    gain = skip[...]

    def gated(left, right):
        return (left[...].astype(F32) * right[...].astype(F32)).astype(BF).astype(F32)

    out[...] = (fq[...].astype(F32) * (spread[:rows, :] + gain * gated(fk, fv))).astype(BF)
    mixed = spread[rows : 2 * rows, :] + gain * gated(bk, bv)
    g_query[...] = (bg[...].astype(F32) * mixed).astype(BF)
    through = spread[2 * rows :, :] + gain * gated(bg, bq)
    g_key[...] = (through * bv[...].astype(F32)).astype(BF)
    g_value[...] = (through * bk[...].astype(F32)).astype(BF)


def finish(plan, scale, arrays, skip, messages):
    rows, width = plan.rows, plan.width
    return pl.pallas_call(
        lambda *refs: finish_kernel(plan, scale, *refs),
        in_specs=[VMEM_SPEC] * (8 + plan.seq),
        out_specs=[VMEM_SPEC] * 6,
        out_shape=[jax.ShapeDtypeStruct((rows, width), BF)] * 4
        + [jax.ShapeDtypeStruct((rows, plan.filt), F32), jax.ShapeDtypeStruct((1, width), F32)],
        scratch_shapes=[pltpu.VMEM((3 * rows, width), F32), pltpu.VMEM((8, width), F32)],
        compiler_params=LIMIT,
        name="finish",
    )(*arrays, skip, *messages)


def swap(value, axis, size, distance):
    return lax.ppermute(value, axis, [(i, i ^ distance) for i in range(size)])


def exchange(values, axis, order):
    size = len(values)
    got = {0: values[0]}
    for d in order:
        got[d] = swap(values[d], axis, size, d)
    return [got[d] for d in range(size)]


def dense_device(plan, fwd_q, fwd_k, fwd_v, bwd_q, bwd_k, bwd_v, bwd_grad, filters, skip):
    scale = 1.0 / math.sqrt(plan.length)
    far_first = list(range(2, plan.seq)) + [1]
    gates = (fwd_k, fwd_v, bwd_k, bwd_v, bwd_grad, bwd_q)
    messages = pack_messages(plan, gates, filters)
    tables = make_tables(plan)
    messages = exchange(messages, "seq", far_first)
    mine = collect_filters(plan, messages)
    pieces = exchange([mine] * plan.chan, "chan", range(1, plan.chan))
    spec, *rest = early_transforms(plan, tables, messages)
    strips, dots = rest[:-1], rest[-1]
    strips = exchange(strips, "chan", range(1, plan.chan))
    results = late_transforms(plan, tables, spec, dots, messages, pieces)
    results = merge_strips(plan, results, strips)
    results = exchange(results, "seq", far_first)
    arrays = (fwd_q, fwd_k, fwd_v, bwd_q, bwd_k, bwd_v, bwd_grad)
    out, g_query, g_key, g_value, g_filter, g_skip = finish(
        plan, scale, arrays, skip.reshape(1, -1), results
    )
    return out, g_query, g_key, g_value, g_filter, g_skip.reshape(-1)


def per_device(*arrays):
    rows, width = arrays[0].shape
    plan = Plan(rows, width, arrays[7].shape[1], lax.axis_size("seq"), lax.axis_size("chan"))
    if plan.fits():
        return dense_device(plan, *arrays)
    return staged_device(*arrays)


def solution(mesh):
    return jax.shard_map(
        per_device,
        mesh=mesh,
        in_specs=(
            P("seq", "chan"),
            P("seq", "chan"),
            P("seq", "chan"),
            P("seq", "chan"),
            P("seq", "chan"),
            P("seq", "chan"),
            P("seq", "chan"),
            P("seq", "chan"),
            P("chan"),
        ),
        out_specs=(
            P("seq", "chan"),
            P("seq", "chan"),
            P("seq", "chan"),
            P("seq", "chan"),
            P("seq", "chan"),
            P("chan"),
        ),
        check_vma=False,
    )
```
